32 devices in a mesh: dp: 8 (over y, x, core), pipe: 4 (over z).
Axes of the slice: x: 2, y: 2, z: 4, core: 2. Of those that a mesh axis runs over, the one named last changes fastest.
Arguments:
- embed_grad: bfloat16 [512, 4608], P('dp', 'pipe'), may hold values from -0.35 to 0.35
- ids: int32 [512], P('dp'), may hold values from 0 to 11263
Outputs:
- table_grad: float32 [11264, 4608], P('dp', 'pipe')
The draws below stay inside these ranges and needn't reach their ends.
All inputs are finite; a program needn't handle non-finite values.
Results may differ from the reference program's by a relative error of at most 0.00035.
Values may be sent and summed in bfloat16 or wider, within the bound.
A program may use at most 64 MiB of HBM per device.

```python
import math
import jax
import jax.numpy as jnp
import numpy as np
from jax import lax

D = 4608
VOC_DEV = 1408
TOKENS = 512
VOCAB = 11264
N_DP = 8


def draw_embed_grad(key, part):
    rows = jnp.arange(TOKENS, dtype=jnp.float32)[:, None] / TOKENS
    columns = jnp.arange(D, dtype=jnp.float32)[None, :] / D
    noise = jnp.clip(jax.random.normal(key, (TOKENS, D), jnp.float32), -5.0, 5.0)
    scale = 0.015 * jnp.exp(jnp.log(3.0) * rows) * jnp.exp(jnp.log(1.5) * columns)
    values = noise * scale
    return jnp.clip(values, -0.35, 0.35).astype(jnp.bfloat16)


def with_ends(drawn, key, low, high):
    longest = drawn.shape.index(max(drawn.shape))
    spots = []
    for shift in (0, 1):
        where = [jax.random.randint(jax.random.fold_in(key, axis), (), 0, length) for axis, length in enumerate(drawn.shape)]
        where[longest] = (where[longest] + shift) % drawn.shape[longest]
        spots.append(tuple(where))
    return drawn.at[spots[0]].set(low).at[spots[1]].set(high)


def rank_bounds(amount, slope):
    weights = [(1 << 20) // math.isqrt(standing ** slope) + 1 for standing in range(1, amount + 1)]
    width = 1 + sum(weights) // (1 << 30)
    return np.cumsum(np.array([max(1, weight // width) for weight in weights]))


def ranked_ids(key, extent, amount, lean):
    table = rank_bounds(amount, lean)
    lot = jax.random.randint(jax.random.fold_in(key, 1), extent, 0, int(table[amount - 1]))
    standing = jnp.searchsorted(jnp.asarray(table, jnp.int32), lot, side="right")
    return jax.random.permutation(jax.random.fold_in(key, 2), amount)[standing].astype(jnp.int32)


def setup_inputs(seed: int = 0) -> dict:
    seeds = jax.random.split(jax.random.key(seed), 3)
    embed_grad = draw_embed_grad(jax.random.fold_in(seeds[2], 71), 0)
    ids = with_ends(ranked_ids(seeds[1], (TOKENS,), VOCAB, 2), jax.random.fold_in(seeds[1], 3), 0, VOCAB - 1).astype(jnp.int32)
    return dict(embed_grad=embed_grad, ids=ids)


def reference(embed_grad, ids):
    cotangent = embed_grad.astype(jnp.float32)

    def block_rows(block_index):
        start = block_index * VOC_DEV
        local = ids - start
        inside = (local >= 0) & (local < VOC_DEV)
        segment = jnp.where(inside, local, VOC_DEV).astype(jnp.int32)
        summed = jax.ops.segment_sum(cotangent, segment, VOC_DEV + 1)
        return summed[:VOC_DEV] * math.sqrt(D)
    grad_rows = lax.map(block_rows, jnp.arange(N_DP, dtype=jnp.int32))
    grad_norm = jnp.sqrt(jnp.sum(grad_rows * grad_rows) + 1e-06)
    factor = jnp.minimum(1.0, 0.2 * math.sqrt(TOKENS * D) / grad_norm)
    return (grad_rows * factor).reshape(VOCAB, D)
```

```python
import functools
import math

import jax
import jax.numpy as jnp
from jax import lax
from jax.experimental import pallas as pl
from jax.experimental.pallas import tpu as pltpu
from jax.sharding import PartitionSpec as P

VOC_DEV = 1408
CHUNKS = 4
MESH = pl.DeviceIdType.MESH


def gather_kernel(n_dp, n_pipe, clip, scale, grad_ref, ids_ref, all_ref, row_ref, factor_ref,
                  held, id_held, sums, load_sem, send_sem, recv_sem, sum_send, sum_recv):
    me = lax.axis_index("dp")
    z = lax.axis_index("pipe")
    core = lax.rem(me, 2)
    to_sibling = 1 - 2 * core
    to_x = 2 - 4 * lax.rem(me // 2, 2)
    to_y = 4 - 8 * (me // 4)
    sibling, x_peer, y_peer = me + to_sibling, me + to_x, me + to_y
    diagonal = me + to_x + to_y
    relayed = me + (1 - core) * to_x + core * to_y
    relay_to = me + core * to_x + (1 - core) * to_y
    rows = held.shape[1] // CHUNKS

    load = pltpu.make_async_copy(grad_ref, held.at[me], load_sem.at[0])
    load.start()
    load_ids = pltpu.make_async_copy(ids_ref, id_held.at[me], load_sem.at[1])
    load_ids.start()

    barrier = pltpu.get_barrier_semaphore()
    for peer in (sibling, x_peer, y_peer):
        pl.semaphore_signal(barrier, inc=1, device_id=(peer, z), device_id_type=MESH)
    for step in range(1, n_pipe):
        pl.semaphore_signal(
            barrier, inc=1, device_id=(me, lax.rem(z + step, n_pipe)), device_id_type=MESH
        )
    pl.semaphore_wait(barrier, 3 + n_pipe - 1)
    load_ids.wait()
    load.wait()

    def piece(block, part):
        if part == 0:
            return id_held.at[block]
        return held.at[block, pl.ds((part - 1) * rows, rows)]

    def copy(block, part, target, kind):
        return pltpu.make_async_remote_copy(
            src_ref=piece(block, part), dst_ref=piece(block, part),
            send_sem=send_sem.at[kind, part], recv_sem=recv_sem.at[block, part],
            device_id=(target, z), device_id_type=MESH,
        )

    sent = []

    def send(block, part, target, kind):
        moving = copy(block, part, target, kind)
        moving.start()
        sent.append(moving)

    def arrived(block, part):
        copy(block, part, sibling, 0).wait_recv()

    parts = range(CHUNKS + 1)
    for part in parts:
        send(me, part, relay_to, 0)
        send(me, part, relayed, 1)
        send(me, part, sibling, 2)
    for part in parts:
        arrived(relayed, part)
        send(relayed, part, relay_to, 3)
        send(relayed, part, sibling, 4)
        arrived(relay_to, part)
        send(relay_to, part, sibling, 5)
    arrived(diagonal, 0)
    send(diagonal, 0, sibling, 6)
    for block in (sibling, sibling + to_x, sibling + to_y, sibling + to_x + to_y):
        arrived(block, 0)

    ids = jnp.concatenate([id_held[block] for block in range(n_dp)], axis=1)
    row_ref[...] = ids
    tokens = ids.shape[1]
    columns = []
    for start in range(0, tokens, 128):
        columns.append(
            jnp.broadcast_to(ids[:, start:start + 128].astype(jnp.float32), (128, 128)).T[:, :1]
        )
    column = jnp.concatenate(columns, axis=0)
    same = jnp.where(column == ids.astype(jnp.float32), 1.0, 0.0)
    here = lax.broadcasted_iota(jnp.int32, same.shape, 0)
    other = lax.broadcasted_iota(jnp.int32, same.shape, 1)
    earlier = jnp.sum(jnp.where(other < here, same, 0.0), axis=1, keepdims=True)
    first = jnp.where(earlier == 0.0, same, 0.0).astype(jnp.bfloat16)

    for part in parts[1:]:
        arrived(diagonal, part)
        send(diagonal, part, sibling, 6)
    for block in (sibling, sibling + to_x, sibling + to_y, sibling + to_x + to_y):
        for part in parts[1:]:
            arrived(block, part)

    width = held.shape[2]
    total = jnp.zeros((1, 128), jnp.float32)
    tile = 384 if width % 384 == 0 else 128
    for start in range(0, width, tile):
        block = held[:, :, start:start + tile].reshape(tokens, tile)
        summed = jnp.dot(first, block, preferred_element_type=jnp.float32)
        squares = jnp.sum(summed * summed, axis=0, keepdims=True)
        for lane in range(0, tile, 128):
            total = total + squares[:, lane:lane + 128]
    sums[z] = total
    shares = []
    for step in range(1, n_pipe):
        share = pltpu.make_async_remote_copy(
            src_ref=sums.at[z], dst_ref=sums.at[z],
            send_sem=sum_send.at[step], recv_sem=sum_recv.at[z],
            device_id=(me, lax.rem(z + step, n_pipe)), device_id_type=MESH,
        )
        share.start()
        shares.append(share)
    all_ref[...] = held[...]
    for step in range(1, n_pipe):
        origin = lax.rem(z + step, n_pipe)
        pltpu.make_async_remote_copy(
            src_ref=sums.at[origin], dst_ref=sums.at[origin],
            send_sem=sum_send.at[step], recv_sem=sum_recv.at[origin],
            device_id=(me, origin), device_id_type=MESH,
        ).wait_recv()
    whole = sums[0]
    for index in range(1, n_pipe):
        whole = whole + sums[index]
    norm = jnp.sqrt(jnp.sum(whole, axis=1, keepdims=True) * (scale * scale) + 1e-06)
    factor = jnp.minimum(1.0, clip / norm) * scale
    factor_ref[...] = jnp.broadcast_to(factor, factor_ref.shape)
    for moving in sent:
        moving.wait_send()
    for share in shares:
        share.wait_send()


def rows_kernel(ids_ref, factor_ref, all_ref, out_ref):
    height = out_ref.shape[0]
    first = lax.axis_index("dp") * VOC_DEV + pl.program_id(0) * height
    tokens = ids_ref.shape[1]
    wanted = lax.broadcasted_iota(jnp.int32, (height, tokens), 0) + first
    hot = jnp.where(wanted == ids_ref[...], 1.0, 0.0).astype(jnp.bfloat16)
    block = all_ref[...].reshape(tokens, all_ref.shape[2])
    summed = jnp.dot(hot, block, preferred_element_type=jnp.float32)
    out_ref[...] = summed * factor_ref[:, :1]


def rows_of(all_grads, ids, factor, height):
    n_dp, count, width = all_grads.shape
    tokens = n_dp * count
    return pl.pallas_call(
        rows_kernel,
        grid=(VOC_DEV // height,),
        out_shape=jax.ShapeDtypeStruct((VOC_DEV, width), jnp.float32),
        in_specs=[
            pl.BlockSpec((1, tokens), lambda i: (0, 0)),
            pl.BlockSpec((1, 128), lambda i: (0, 0)),
            pl.BlockSpec((n_dp, count, width), lambda i: (0, 0, 0)),
        ],
        out_specs=pl.BlockSpec((height, width), lambda i: (i, 0)),
        compiler_params=pltpu.CompilerParams(dimension_semantics=("arbitrary",)),
        cost_estimate=pl.CostEstimate(
            flops=2 * VOC_DEV * tokens * width, bytes_accessed=4 * VOC_DEV * width, transcendentals=0
        ),
        name="rows",
    )(ids, factor, all_grads)


def per_device(embed_grad, ids):
    n_dp, n_pipe = lax.axis_size("dp"), lax.axis_size("pipe")
    count, width = embed_grad.shape
    features = width * n_pipe
    tokens = count * n_dp
    vmem = pl.BlockSpec(memory_space=pltpu.VMEM)
    any_space = pl.BlockSpec(memory_space=pl.ANY)
    all_grads, all_ids, factor = pl.pallas_call(
        functools.partial(
            gather_kernel, n_dp, n_pipe, 0.2 * math.sqrt(tokens * features), math.sqrt(features)
        ),
        out_shape=(
            jax.ShapeDtypeStruct((n_dp, count, width), embed_grad.dtype),
            jax.ShapeDtypeStruct((1, tokens), jnp.int32),
            jax.ShapeDtypeStruct((1, 128), jnp.float32),
        ),
        in_specs=[any_space, any_space],
        out_specs=(vmem, vmem, vmem),
        scratch_shapes=[
            pltpu.VMEM((n_dp, count, width), embed_grad.dtype),
            pltpu.VMEM((n_dp, 1, count), jnp.int32),
            pltpu.VMEM((n_pipe, 1, 128), jnp.float32),
            pltpu.SemaphoreType.DMA((2,)),
            pltpu.SemaphoreType.DMA((7, CHUNKS + 1)),
            pltpu.SemaphoreType.DMA((n_dp, CHUNKS + 1)),
            pltpu.SemaphoreType.DMA((n_pipe,)),
            pltpu.SemaphoreType.DMA((n_pipe,)),
        ],
        compiler_params=pltpu.CompilerParams(collective_id=0, has_side_effects=True),
        name="gather",
    )(embed_grad, ids.reshape(1, count))
    return rows_of(all_grads, all_ids, factor, VOC_DEV // 8)


def per_device_any(embed_grad, ids):
    tokens_all = embed_grad.shape[0] * lax.axis_size("dp")
    features = embed_grad.shape[1] * lax.axis_size("pipe")
    offset = lax.axis_index("dp") * VOC_DEV
    cotangent_all = lax.all_gather(embed_grad, "dp", axis=0, tiled=True)
    local = lax.all_gather(ids, "dp", axis=0, tiled=True) - offset
    inside = (local >= 0) & (local < VOC_DEV)
    segment = jnp.where(inside, local, VOC_DEV).astype(jnp.int32)
    summed = jax.ops.segment_sum(cotangent_all.astype(jnp.float32), segment, VOC_DEV + 1)
    grad_rows = summed[:VOC_DEV] * math.sqrt(features)
    total = lax.psum(jnp.sum(grad_rows * grad_rows), ("dp", "pipe"))
    grad_norm = jnp.sqrt(total + 1e-06)
    return grad_rows * jnp.minimum(1.0, 0.2 * math.sqrt(tokens_all * features) / grad_norm)


def solution(mesh):
    placed = (P("dp", "pipe"), P("dp"))
    cube = mesh.shape["dp"] == 2 * 2 * 2
    return jax.shard_map(
        per_device if cube else per_device_any, mesh=mesh, in_specs=placed,
        out_specs=P("dp", "pipe"), check_vma=False,
    )
```

```python
import functools
import math

import jax
import jax.numpy as jnp
from jax import lax
from jax.experimental import pallas as pl
from jax.experimental.pallas import tpu as pltpu
from jax.sharding import PartitionSpec as P

VOC_DEV = 1408
CHUNKS = 4
STRIPES = 8
MESH = pl.DeviceIdType.MESH


def gather_kernel(n_dp, n_pipe, clip, scale, grad_ref, ids_ref, all_ref, row_ref, factor_ref,
                  held, id_held, sums, load_sem, send_sem, recv_sem, sum_send, sum_recv):
    me = lax.axis_index("dp")
    z = lax.axis_index("pipe")
    core = lax.rem(me, 2)
    to_sibling = 1 - 2 * core
    to_x = 2 - 4 * lax.rem(me // 2, 2)
    to_y = 4 - 8 * (me // 4)
    sibling, x_peer, y_peer = me + to_sibling, me + to_x, me + to_y
    diagonal = me + to_x + to_y
    relayed = me + (1 - core) * to_x + core * to_y
    relay_to = me + core * to_x + (1 - core) * to_y
    rows = held.shape[1] // CHUNKS

    load = pltpu.make_async_copy(grad_ref, held.at[me], load_sem.at[0])
    load.start()
    load_ids = pltpu.make_async_copy(ids_ref, id_held.at[me], load_sem.at[1])
    load_ids.start()

    barrier = pltpu.get_barrier_semaphore()
    for peer in (sibling, x_peer, y_peer):
        pl.semaphore_signal(barrier, inc=1, device_id=(peer, z), device_id_type=MESH)
    for step in range(1, n_pipe):
        pl.semaphore_signal(
            barrier, inc=1, device_id=(me, lax.rem(z + step, n_pipe)), device_id_type=MESH
        )
    pl.semaphore_wait(barrier, 3 + n_pipe - 1)
    load_ids.wait()
    load.wait()

    def piece(block, part):
        if part == 0:
            return id_held.at[block]
        return held.at[block, pl.ds((part - 1) * rows, rows)]

    def copy(block, part, target, kind):
        return pltpu.make_async_remote_copy(
            src_ref=piece(block, part), dst_ref=piece(block, part),
            send_sem=send_sem.at[kind, part], recv_sem=recv_sem.at[block, part],
            device_id=(target, z), device_id_type=MESH,
        )

    sent = []

    def send(block, part, target, kind):
        moving = copy(block, part, target, kind)
        moving.start()
        sent.append(moving)

    def arrived(block, part):
        copy(block, part, sibling, 0).wait_recv()

    parts = range(CHUNKS + 1)
    for part in parts:
        send(me, part, relay_to, 0)
        send(me, part, relayed, 1)
        send(me, part, sibling, 2)
    for part in parts:
        arrived(relayed, part)
        send(relayed, part, relay_to, 3)
        send(relayed, part, sibling, 4)
        arrived(relay_to, part)
        send(relay_to, part, sibling, 5)
    arrived(diagonal, 0)
    send(diagonal, 0, sibling, 6)
    for block in (sibling, sibling + to_x, sibling + to_y, sibling + to_x + to_y):
        arrived(block, 0)

    ids = jnp.concatenate([id_held[block] for block in range(n_dp)], axis=1)
    row_ref[...] = ids
    tokens = ids.shape[1]
    columns = []
    for start in range(0, tokens, 128):
        columns.append(
            jnp.broadcast_to(ids[:, start:start + 128].astype(jnp.float32), (128, 128)).T[:, :1]
        )
    column = jnp.concatenate(columns, axis=0)
    same = jnp.where(column == ids.astype(jnp.float32), 1.0, 0.0)
    here = lax.broadcasted_iota(jnp.int32, same.shape, 0)
    other = lax.broadcasted_iota(jnp.int32, same.shape, 1)
    earlier = jnp.sum(jnp.where(other < here, same, 0.0), axis=1, keepdims=True)
    first = jnp.where(earlier == 0.0, same, 0.0).astype(jnp.bfloat16)

    for part in parts[1:]:
        arrived(diagonal, part)
        send(diagonal, part, sibling, 6)
    for block in (sibling, sibling + to_x, sibling + to_y, sibling + to_x + to_y):
        for part in parts[1:]:
            arrived(block, part)

    width = held.shape[2]
    total = jnp.zeros((1, 128), jnp.float32)
    tile = 384 if width % 384 == 0 else 128
    for start in range(0, width, tile):
        block = held[:, :, start:start + tile].reshape(tokens, tile)
        summed = jnp.dot(first, block, preferred_element_type=jnp.float32)
        squares = jnp.sum(summed * summed, axis=0, keepdims=True)
        for lane in range(0, tile, 128):
            total = total + squares[:, lane:lane + 128]
    sums[z] = total
    shares = []
    for step in range(1, n_pipe):
        share = pltpu.make_async_remote_copy(
            src_ref=sums.at[z], dst_ref=sums.at[z],
            send_sem=sum_send.at[step], recv_sem=sum_recv.at[z],
            device_id=(me, lax.rem(z + step, n_pipe)), device_id_type=MESH,
        )
        share.start()
        shares.append(share)
    all_ref[...] = held[...]
    for step in range(1, n_pipe):
        origin = lax.rem(z + step, n_pipe)
        pltpu.make_async_remote_copy(
            src_ref=sums.at[origin], dst_ref=sums.at[origin],
            send_sem=sum_send.at[step], recv_sem=sum_recv.at[origin],
            device_id=(me, origin), device_id_type=MESH,
        ).wait_recv()
    whole = sums[0]
    for index in range(1, n_pipe):
        whole = whole + sums[index]
    norm = jnp.sqrt(jnp.sum(whole, axis=1, keepdims=True) * (scale * scale) + 1e-06)
    factor = jnp.minimum(1.0, clip / norm) * scale
    factor_ref[...] = jnp.broadcast_to(factor, factor_ref.shape)
    for moving in sent:
        moving.wait_send()
    for share in shares:
        share.wait_send()


def rows_kernel(ids_ref, factor_ref, all_ref, out_ref, made, sem):
    height = made.shape[0] // STRIPES
    tokens = ids_ref.shape[1]
    offset = lax.axis_index("dp") * VOC_DEV
    block = all_ref[...].reshape(tokens, all_ref.shape[2])
    factor = factor_ref[:, :1]
    writes = []
    for stripe in range(STRIPES):
        where = pl.ds(stripe * height, height)
        wanted = lax.broadcasted_iota(jnp.int32, (height, tokens), 0) + (offset + stripe * height)
        hot = jnp.where(wanted == ids_ref[...], 1.0, 0.0).astype(jnp.bfloat16)
        made[where] = jnp.dot(hot, block, preferred_element_type=jnp.float32) * factor
        write = pltpu.make_async_copy(made.at[where], out_ref.at[where], sem.at[stripe])
        write.start()
        writes.append(write)
    for write in writes:
        write.wait()


def rows_of(all_grads, ids, factor):
    n_dp, count, width = all_grads.shape
    vmem = pl.BlockSpec(memory_space=pltpu.VMEM)
    return pl.pallas_call(
        rows_kernel,
        out_shape=jax.ShapeDtypeStruct((VOC_DEV, width), jnp.float32),
        in_specs=[vmem, vmem, vmem],
        out_specs=pl.BlockSpec(memory_space=pltpu.HBM),
        scratch_shapes=[
            pltpu.VMEM((VOC_DEV, width), jnp.float32),
            pltpu.SemaphoreType.DMA((STRIPES,)),
        ],
        compiler_params=pltpu.CompilerParams(vmem_limit_bytes=24 * 2**20),
        name="rows",
    )(ids, factor, all_grads)


def per_device(embed_grad, ids):
    n_dp, n_pipe = lax.axis_size("dp"), lax.axis_size("pipe")
    count, width = embed_grad.shape
    features = width * n_pipe
    tokens = count * n_dp
    vmem = pl.BlockSpec(memory_space=pltpu.VMEM)
    hbm = pl.BlockSpec(memory_space=pltpu.HBM)
    all_grads, all_ids, factor = pl.pallas_call(
        functools.partial(
            gather_kernel, n_dp, n_pipe, 0.2 * math.sqrt(tokens * features), math.sqrt(features)
        ),
        out_shape=(
            pltpu.VMEM((n_dp, count, width), embed_grad.dtype),
            pltpu.VMEM((1, tokens), jnp.int32),
            pltpu.VMEM((1, 128), jnp.float32),
        ),
        in_specs=[hbm, hbm],
        out_specs=(vmem, vmem, vmem),
        scratch_shapes=[
            pltpu.VMEM((n_dp, count, width), embed_grad.dtype),
            pltpu.VMEM((n_dp, 1, count), jnp.int32),
            pltpu.VMEM((n_pipe, 1, 128), jnp.float32),
            pltpu.SemaphoreType.DMA((2,)),
            pltpu.SemaphoreType.DMA((7, CHUNKS + 1)),
            pltpu.SemaphoreType.DMA((n_dp, CHUNKS + 1)),
            pltpu.SemaphoreType.DMA((n_pipe,)),
            pltpu.SemaphoreType.DMA((n_pipe,)),
        ],
        compiler_params=pltpu.CompilerParams(
            collective_id=0, has_side_effects=True, vmem_limit_bytes=24 * 2**20
        ),
        name="gather",
    )(embed_grad, ids.reshape(1, count))
    return rows_of(all_grads, all_ids, factor)


def per_device_any(embed_grad, ids):
    tokens_all = embed_grad.shape[0] * lax.axis_size("dp")
    features = embed_grad.shape[1] * lax.axis_size("pipe")
    offset = lax.axis_index("dp") * VOC_DEV
    cotangent_all = lax.all_gather(embed_grad, "dp", axis=0, tiled=True)
    local = lax.all_gather(ids, "dp", axis=0, tiled=True) - offset
    inside = (local >= 0) & (local < VOC_DEV)
    segment = jnp.where(inside, local, VOC_DEV).astype(jnp.int32)
    summed = jax.ops.segment_sum(cotangent_all.astype(jnp.float32), segment, VOC_DEV + 1)
    grad_rows = summed[:VOC_DEV] * math.sqrt(features)
    total = lax.psum(jnp.sum(grad_rows * grad_rows), ("dp", "pipe"))
    grad_norm = jnp.sqrt(total + 1e-06)
    return grad_rows * jnp.minimum(1.0, 0.2 * math.sqrt(tokens_all * features) / grad_norm)


def solution(mesh):
    placed = (P("dp", "pipe"), P("dp"))
    cube = mesh.shape["dp"] == 2 * 2 * 2
    return jax.shard_map(
        per_device if cube else per_device_any, mesh=mesh, in_specs=placed,
        out_specs=P("dp", "pipe"), check_vma=False,
    )
```

```python
import functools
import math

import jax
import jax.numpy as jnp
from jax import lax
from jax.experimental import pallas as pl
from jax.experimental.pallas import tpu as pltpu
from jax.sharding import PartitionSpec as P

VOC_DEV = 1408
CHUNKS = 4
STRIPES = 8
MESH = pl.DeviceIdType.MESH


def gather_kernel(n_dp, n_pipe, clip, scale, grad_ref, ids_ref, all_ref, row_ref, factor_ref,
                  held, id_held, sums, load_sem, send_sem, recv_sem, sum_send, sum_recv):
    me = lax.axis_index("dp")
    z = lax.axis_index("pipe")
    core = lax.rem(me, 2)
    to_sibling = 1 - 2 * core
    to_x = 2 - 4 * lax.rem(me // 2, 2)
    to_y = 4 - 8 * (me // 4)
    sibling, x_peer, y_peer = me + to_sibling, me + to_x, me + to_y
    diagonal = me + to_x + to_y
    relayed = me + (1 - core) * to_x + core * to_y
    relay_to = me + core * to_x + (1 - core) * to_y
    rows = held.shape[1] // CHUNKS

    load = pltpu.make_async_copy(grad_ref, held.at[me], load_sem.at[0])
    load.start()
    load_ids = pltpu.make_async_copy(ids_ref, id_held.at[me], load_sem.at[1])
    load_ids.start()

    barrier = pltpu.get_barrier_semaphore()
    for peer in (sibling, x_peer, y_peer):
        pl.semaphore_signal(barrier, inc=1, device_id=(peer, z), device_id_type=MESH)
    for step in range(1, n_pipe):
        pl.semaphore_signal(
            barrier, inc=1, device_id=(me, lax.rem(z + step, n_pipe)), device_id_type=MESH
        )
    pl.semaphore_wait(barrier, 3 + n_pipe - 1)
    load_ids.wait()
    load.wait()

    def piece(block, part):
        if part == 0:
            return id_held.at[block]
        return held.at[block, pl.ds((part - 1) * rows, rows)]

    def copy(block, part, target, kind):
        return pltpu.make_async_remote_copy(
            src_ref=piece(block, part), dst_ref=piece(block, part),
            send_sem=send_sem.at[kind, part], recv_sem=recv_sem.at[block, part],
            device_id=(target, z), device_id_type=MESH,
        )

    sent = []

    def send(block, part, target, kind):
        moving = copy(block, part, target, kind)
        moving.start()
        sent.append(moving)

    def arrived(block, part):
        copy(block, part, sibling, 0).wait_recv()

    parts = range(CHUNKS + 1)
    for part in parts:
        send(me, part, relay_to, 0)
        send(me, part, relayed, 1)
        send(me, part, sibling, 2)
    for part in parts:
        arrived(relayed, part)
        send(relayed, part, relay_to, 3)
        send(relayed, part, sibling, 4)
        arrived(relay_to, part)
        send(relay_to, part, sibling, 5)
    arrived(diagonal, 0)
    send(diagonal, 0, sibling, 6)
    for block in (sibling, sibling + to_x, sibling + to_y, sibling + to_x + to_y):
        arrived(block, 0)

    ids = jnp.concatenate([id_held[block] for block in range(n_dp)], axis=1)
    row_ref[...] = ids
    tokens = ids.shape[1]
    columns = []
    for start in range(0, tokens, 128):
        columns.append(
            jnp.broadcast_to(ids[:, start:start + 128].astype(jnp.float32), (128, 128)).T[:, :1]
        )
    column = jnp.concatenate(columns, axis=0)
    same = jnp.where(column == ids.astype(jnp.float32), 1.0, 0.0)
    here = lax.broadcasted_iota(jnp.int32, same.shape, 0)
    other = lax.broadcasted_iota(jnp.int32, same.shape, 1)
    earlier = jnp.sum(jnp.where(other < here, same, 0.0), axis=1, keepdims=True)
    first = jnp.where(earlier == 0.0, same, 0.0).astype(jnp.bfloat16)

    for part in parts[1:]:
        arrived(diagonal, part)
        send(diagonal, part, sibling, 6)
    for block in (sibling, sibling + to_x, sibling + to_y, sibling + to_x + to_y):
        for part in parts[1:]:
            arrived(block, part)

    width = held.shape[2]
    total = jnp.zeros((1, 128), jnp.float32)
    tile = 384 if width % 384 == 0 else 128
    for start in range(0, width, tile):
        block = held[:, :, start:start + tile].reshape(tokens, tile)
        summed = jnp.dot(first, block, preferred_element_type=jnp.float32)
        squares = jnp.sum(summed * summed, axis=0, keepdims=True)
        for lane in range(0, tile, 128):
            total = total + squares[:, lane:lane + 128]
    sums[z] = total
    shares = []
    for step in range(1, n_pipe):
        share = pltpu.make_async_remote_copy(
            src_ref=sums.at[z], dst_ref=sums.at[z],
            send_sem=sum_send.at[step], recv_sem=sum_recv.at[z],
            device_id=(me, lax.rem(z + step, n_pipe)), device_id_type=MESH,
        )
        share.start()
        shares.append(share)
    all_ref[...] = held[...]
    for step in range(1, n_pipe):
        origin = lax.rem(z + step, n_pipe)
        pltpu.make_async_remote_copy(
            src_ref=sums.at[origin], dst_ref=sums.at[origin],
            send_sem=sum_send.at[step], recv_sem=sum_recv.at[origin],
            device_id=(me, origin), device_id_type=MESH,
        ).wait_recv()
    whole = sums[0]
    for index in range(1, n_pipe):
        whole = whole + sums[index]
    norm = jnp.sqrt(jnp.sum(whole, axis=1, keepdims=True) * (scale * scale) + 1e-06)
    factor = jnp.minimum(1.0, clip / norm) * scale
    factor_ref[...] = jnp.broadcast_to(factor, factor_ref.shape)
    for moving in sent:
        moving.wait_send()
    for share in shares:
        share.wait_send()


def rows_kernel(ids_ref, factor_ref, all_ref, out_ref, made, sem):
    height = made.shape[0] // STRIPES
    tokens = ids_ref.shape[1]
    offset = lax.axis_index("dp") * VOC_DEV
    block = all_ref[...].reshape(tokens, all_ref.shape[2])
    factor = factor_ref[:, :1]
    writes = []
    for stripe in range(STRIPES):
        where = pl.ds(stripe * height, height)
        wanted = lax.broadcasted_iota(jnp.int32, (height, tokens), 0) + (offset + stripe * height)
        hot = jnp.where(wanted == ids_ref[...], 1.0, 0.0).astype(jnp.bfloat16)
        made[where] = jnp.dot(hot, block, preferred_element_type=jnp.float32) * factor
        write = pltpu.make_async_copy(made.at[where], out_ref.at[where], sem.at[stripe])
        write.start()
        writes.append(write)
    for write in writes:
        write.wait()


def rows_of(all_grads, ids, factor):
    n_dp, count, width = all_grads.shape
    vmem = pl.BlockSpec(memory_space=pltpu.VMEM)
    return pl.pallas_call(
        rows_kernel,
        out_shape=jax.ShapeDtypeStruct((VOC_DEV, width), jnp.float32),
        in_specs=[vmem, vmem, vmem],
        out_specs=pl.BlockSpec(memory_space=pltpu.HBM),
        scratch_shapes=[
            pltpu.VMEM((VOC_DEV, width), jnp.float32),
            pltpu.SemaphoreType.DMA((STRIPES,)),
        ],
        compiler_params=pltpu.CompilerParams(vmem_limit_bytes=24 * 2**20),
        name="rows",
    )(ids, factor, all_grads)


def per_device(embed_grad, ids):
    n_dp, n_pipe = lax.axis_size("dp"), lax.axis_size("pipe")
    count, width = embed_grad.shape
    features = width * n_pipe
    tokens = count * n_dp
    vmem = pl.BlockSpec(memory_space=pltpu.VMEM)
    hbm = pl.BlockSpec(memory_space=pltpu.HBM)
    all_grads, all_ids, factor = pl.pallas_call(
        functools.partial(
            gather_kernel, n_dp, n_pipe, 0.2 * math.sqrt(tokens * features), math.sqrt(features)
        ),
        out_shape=(
            pltpu.VMEM((n_dp, count, width), embed_grad.dtype),
            pltpu.VMEM((1, tokens), jnp.int32),
            pltpu.VMEM((1, 128), jnp.float32),
        ),
        in_specs=[hbm, hbm],
        out_specs=(vmem, vmem, vmem),
        scratch_shapes=[
            pltpu.VMEM((n_dp, count, width), embed_grad.dtype),
            pltpu.VMEM((n_dp, 1, count), jnp.int32),
            pltpu.VMEM((n_pipe, 1, 128), jnp.float32),
            pltpu.SemaphoreType.DMA((2,)),
            pltpu.SemaphoreType.DMA((7, CHUNKS + 1)),
            pltpu.SemaphoreType.DMA((n_dp, CHUNKS + 1)),
            pltpu.SemaphoreType.DMA((n_pipe,)),
            pltpu.SemaphoreType.DMA((n_pipe,)),
        ],
        compiler_params=pltpu.CompilerParams(
            collective_id=0, has_side_effects=True, vmem_limit_bytes=24 * 2**20
        ),
        name="gather",
    )(
        pltpu.with_memory_space_constraint(embed_grad, pltpu.HBM),
        pltpu.with_memory_space_constraint(ids.reshape(1, count), pltpu.HBM),
    )
    return rows_of(all_grads, all_ids, factor)


def per_device_any(embed_grad, ids):
    tokens_all = embed_grad.shape[0] * lax.axis_size("dp")
    features = embed_grad.shape[1] * lax.axis_size("pipe")
    offset = lax.axis_index("dp") * VOC_DEV
    cotangent_all = lax.all_gather(embed_grad, "dp", axis=0, tiled=True)
    local = lax.all_gather(ids, "dp", axis=0, tiled=True) - offset
    inside = (local >= 0) & (local < VOC_DEV)
    segment = jnp.where(inside, local, VOC_DEV).astype(jnp.int32)
    summed = jax.ops.segment_sum(cotangent_all.astype(jnp.float32), segment, VOC_DEV + 1)
    grad_rows = summed[:VOC_DEV] * math.sqrt(features)
    total = lax.psum(jnp.sum(grad_rows * grad_rows), ("dp", "pipe"))
    grad_norm = jnp.sqrt(total + 1e-06)
    return grad_rows * jnp.minimum(1.0, 0.2 * math.sqrt(tokens_all * features) / grad_norm)


def solution(mesh):
    placed = (P("dp", "pipe"), P("dp"))
    cube = mesh.shape["dp"] == 2 * 2 * 2
    return jax.shard_map(
        per_device if cube else per_device_any, mesh=mesh, in_specs=placed,
        out_specs=P("dp", "pipe"), check_vma=False,
    )
```
